32 devices in a mesh: dom: 8 (over z, x), dp: 4 (over y, core).
Axes of the slice: x: 2, y: 2, z: 4, core: 2. Of those that a mesh axis runs over, the one named last changes fastest.
Arguments:
- node_latents: bfloat16 [32768, 128], P(('dom', 'dp')), may hold values from -6 to 6
- mesh_latents: bfloat16 [98304, 128], P(('dom', 'dp')), may hold values from -6 to 6
- world_latents: bfloat16 [16384, 128], P(('dom', 'dp')), may hold values from -6 to 6
- mesh_src: int32 [98304], P(('dom', 'dp')), may hold values from 0 to 1535, as said below
- mesh_dst: int32 [98304], P(('dom', 'dp')), may hold values from 0 to 1023
- world_src: int32 [16384], P(('dom', 'dp')), may hold values from 0 to 2047, as said below
- world_dst: int32 [16384], P(('dom', 'dp')), may hold values from 0 to 1023
- send_blocks: int32 [32, 8, 16], P(('dom', 'dp')), may hold values from 0 to 63
- world_count: int32 [32], P(('dom', 'dp')), may hold values from 256 to 512, as said below
- node_cot: bfloat16 [32768, 128], P(('dom', 'dp')), may hold values from -6 to 6
- mesh_cot: bfloat16 [98304, 128], P(('dom', 'dp')), may hold values from -6 to 6
- world_cot: bfloat16 [16384, 128], P(('dom', 'dp')), may hold values from -6 to 6
- first_weights: bfloat16 [3, 384, 128], replicated, may hold values from -0.3125 to 0.3125
- rest_weights: bfloat16 [3, 2, 128, 128], replicated, may hold values from -0.5 to 0.5
- biases: float32 [3, 4, 128], replicated, may hold values from -2 to 2
- gains: float32 [3, 128], replicated, may hold values from 0.1 to 1.9
Outputs:
- new_nodes: bfloat16 [32768, 128], P(('dom', 'dp'))
- new_mesh: bfloat16 [98304, 128], P(('dom', 'dp'))
- new_world: bfloat16 [16384, 128], P(('dom', 'dp'))
- grad_nodes: bfloat16 [32768, 128], P(('dom', 'dp'))
- grad_mesh: bfloat16 [98304, 128], P(('dom', 'dp'))
- grad_world: bfloat16 [16384, 128], P(('dom', 'dp'))
- grad_first: float32 [3, 384, 128], replicated
- grad_rest: float32 [3, 2, 128, 128], replicated
- grad_biases: float32 [3, 4, 128], replicated
- grad_gains: float32 [3, 128], replicated
The draws below stay inside these ranges and needn't reach their ends.
Inputs may be any that keep to these rules, and one draw needn't show every extreme that they name: `mesh_src`: indexes the 256 rows before a partition's nodes (the last rows of the previous domain of its mesh), its 1024 nodes, then the 256 rows after (the first rows of the next domain); the first domain reads no rows before and the last none after. `world_src`: row j of slot t of the blocks sent by domain p of the same mesh is (p * 16 + t) * 16 + j; a partition reads some slots of each domain, all 16 for at least one. send_blocks[k, p, t] is the block of 16 node rows of partition k put in slot t for domain p of its mesh. Rows of partition k at or past world_count[k] are padding; some partition has all 512 rows live.
All inputs are finite; a program needn't handle non-finite values.
Results may differ from the reference program's by a relative error of at most 0.007.
Values may be sent and summed in bfloat16 or wider, within the bound.
No kernel may reach another device: no remote copies, remote signals or barrier semaphores. Data moves between devices by JAX's collectives and lax.ppermute only.
A program may use at most 128 MiB of HBM per device.

```python
import jax
import jax.numpy as jnp
from jax import lax

D = 128
NODE_DEV = 1024
HALO = 256
BLK = 16
SLOTS = 16
MEDGE_DEV = 3072
WEDGE_DEV = 512
NODES = 32768
MEDGES = 98304
WEDGES = 16384
N_DOM = 8
N_DP = 4


def draw_mesh_src(key, part):
    key = jax.random.fold_in(key, 11)
    key_pick, key_left, key_right, key_inner = jax.random.split(key, 4)
    total_rows = MEDGE_DEV * N_DOM * N_DP
    device = jnp.arange(total_rows, dtype=jnp.int32) // MEDGE_DEV
    domain = device // N_DP
    picked = jax.random.randint(key_pick, (total_rows,), 0, 8)
    left_rows = jax.random.randint(key_left, (total_rows,), 0, HALO)
    right_rows = HALO + NODE_DEV + jax.random.randint(key_right, (total_rows,), 0, HALO)
    inner_rows = HALO + jax.random.randint(key_inner, (total_rows,), 0, NODE_DEV)
    chosen = jnp.where((picked == 0) & (domain > 0), left_rows, jnp.where((picked == 1) & (domain < N_DOM - 1), right_rows, inner_rows))
    return chosen.astype(jnp.int32)


def draw_world_src(key, part):
    key = jax.random.fold_in(key, 37)
    key_live, key_full, key_peer, key_slot, key_row = jax.random.split(key, 5)
    device_count = N_DOM * N_DP
    total_rows = WEDGE_DEV * device_count
    device = jnp.arange(total_rows, dtype=jnp.int32) // WEDGE_DEV
    live_slots = jax.random.randint(key_live, (device_count, N_DOM), 1, SLOTS + 1)
    full_peer = jax.random.randint(key_full, (device_count,), 0, N_DOM)
    live_slots = jnp.where(jnp.arange(N_DOM, dtype=jnp.int32)[None, :] == full_peer[:, None], SLOTS, live_slots)
    peer = jax.random.randint(key_peer, (total_rows,), 0, N_DOM)
    slot = jax.random.randint(key_slot, (total_rows,), 0, 65520) % live_slots[device, peer]
    row_within = jax.random.randint(key_row, (total_rows,), 0, BLK)
    return ((peer * SLOTS + slot) * BLK + row_within).astype(jnp.int32)


def draw_world_count(key, part):
    key = jax.random.fold_in(key, 23)
    key_one, key_top = jax.random.split(key, 2)
    device_count = N_DOM * N_DP
    counted = jax.random.randint(key_one, (device_count,), WEDGE_DEV // 2, WEDGE_DEV + 1)
    busiest = jax.random.randint(key_top, (), 0, device_count)
    counted = jnp.where(jnp.arange(device_count, dtype=jnp.int32) == busiest, WEDGE_DEV, counted)
    return counted.astype(jnp.int32)


def touch_ends(entries, key, low, largest):
    extent = entries.shape
    spot = [jax.random.randint(jax.random.fold_in(key, axis), (), 0, extent[axis]) for axis in range(len(extent))]
    entries = entries.at[tuple(spot)].set(low)
    longest = extent.index(max(extent))
    spot[longest] = (spot[longest] + 1) % extent[longest]
    return entries.at[tuple(spot)].set(largest)


def level_of(own_key, dims, pieces, low, top_value):
    gain, own = 1.0, jax.random.fold_in(own_key, 6)
    for axis_at, shards_of in pieces:
        heights = jnp.exp(jax.random.uniform(jax.random.fold_in(own, axis_at), (shards_of,), jnp.float32, low / len(pieces), top_value / len(pieces)))
        gain = gain * jnp.repeat(heights, dims[axis_at] // shards_of).reshape([-1 if axis == axis_at else 1 for axis in range(len(dims))])
    return gain


def normal_values(rng, shape, width, most, shards=(), kind=jnp.bfloat16):
    entries = jax.random.normal(rng, shape, jnp.float32) * width
    if len(shards) > 0:
        entries = level_of(rng, shape, shards, -0.22, 0.18) * entries
    return jnp.clip(entries, min=-most, max=most).astype(kind)


def setup_inputs(seed: int = 0) -> dict:
    seeds = jax.random.split(jax.random.key(seed), 17)
    node_latents = normal_values(seeds[0], (NODES, D), 1.0, 6.0, ((0, 32),))
    mesh_latents = normal_values(seeds[1], (MEDGES, D), 1.0, 6.0, ((0, 32),))
    world_latents = normal_values(seeds[2], (WEDGES, D), 1.0, 6.0, ((0, 32),))
    mesh_src = draw_mesh_src(jax.random.fold_in(seeds[16], 71), 0)
    mesh_dst = touch_ends(jax.random.randint(seeds[4], (MEDGES,), 0, NODE_DEV), jax.random.fold_in(seeds[4], 1), 0, NODE_DEV - 1).astype(jnp.int32)
    world_src = draw_world_src(jax.random.fold_in(seeds[16], 71), 0)
    world_dst = touch_ends(jax.random.randint(seeds[6], (WEDGES,), 0, NODE_DEV), jax.random.fold_in(seeds[6], 1), 0, NODE_DEV - 1).astype(jnp.int32)
    send_blocks = touch_ends(jax.random.randint(seeds[7], (N_DOM * N_DP, N_DOM, SLOTS), 0, NODE_DEV // BLK), jax.random.fold_in(seeds[7], 1), 0, (NODE_DEV // BLK) - 1).astype(jnp.int32)
    world_count = draw_world_count(jax.random.fold_in(seeds[16], 71), 0)
    node_cot = normal_values(seeds[9], (NODES, D), 1.0, 6.0, ((0, 32),))
    mesh_cot = normal_values(seeds[10], (MEDGES, D), 1.0, 6.0, ((0, 32),))
    world_cot = normal_values(seeds[11], (WEDGES, D), 1.0, 6.0, ((0, 32),))
    first_weights = normal_values(seeds[12], (3, 3 * D, D), (3 * D) ** -0.5, 0.3125)
    rest_weights = normal_values(seeds[13], (3, 2, D, D), D ** -0.5, 0.5)
    biases = normal_values(seeds[14], (3, 4, D), 0.3, 2.0, (), jnp.float32)
    gains = jnp.clip(1.0 + 0.18 * jax.random.normal(seeds[15], (3, D), jnp.float32), 0.1, 1.9)
    return dict(node_latents=node_latents, mesh_latents=mesh_latents, world_latents=world_latents, mesh_src=mesh_src, mesh_dst=mesh_dst, world_src=world_src, world_dst=world_dst, send_blocks=send_blocks, world_count=world_count, node_cot=node_cot, mesh_cot=mesh_cot, world_cot=world_cot, first_weights=first_weights, rest_weights=rest_weights, biases=biases, gains=gains)


norm_eps = 1e-05

def matmul(left, right):
    return jnp.dot(left, right, preferred_element_type=jnp.float32)

def matmul_nt(left, right):
    return lax.dot_general(left, right, (((1,), (1,)), ((), ())), preferred_element_type=jnp.float32)

def matmul_tn(left, right):
    return lax.dot_general(left, right, (((0,), (0,)), ((), ())), preferred_element_type=jnp.float32)

def silu_grad(values):
    sigma = jax.nn.sigmoid(values)
    return sigma * (1.0 + values * (1.0 - sigma))

def mlp_parts(inputs, first_w, rest_w, bias_rows, gain_row):
    pre_one = matmul(inputs, first_w) + bias_rows[0]
    act_one = jax.nn.silu(pre_one).astype(jnp.bfloat16)
    pre_two = matmul(act_one, rest_w[0]) + bias_rows[1]
    act_two = jax.nn.silu(pre_two).astype(jnp.bfloat16)
    pre_three = matmul(act_two, rest_w[1]) + bias_rows[2]
    centred = pre_three - lax.optimization_barrier(jnp.mean(pre_three, axis=-1, keepdims=True))
    inv_std = lax.rsqrt(lax.optimization_barrier(jnp.mean(centred * centred, axis=-1, keepdims=True)) + norm_eps)
    normed = centred * inv_std
    output = normed * gain_row + bias_rows[3]
    return (output, (pre_one, act_one, pre_two, act_two, normed, inv_std))

def mlp_backward(inputs, first_w, rest_w, bias_rows, gain_row, cotangent):
    _, saved = mlp_parts(inputs, first_w, rest_w, bias_rows, gain_row)
    pre_one, act_one, pre_two, act_two, normed, inv_std = saved
    grad_gain = lax.optimization_barrier(jnp.sum(cotangent * normed, axis=0))
    grad_shift = lax.optimization_barrier(jnp.sum(cotangent, axis=0))
    scaled = cotangent * gain_row
    d_three = inv_std * (scaled - lax.optimization_barrier(jnp.mean(scaled, axis=-1, keepdims=True)) - normed * lax.optimization_barrier(jnp.mean(scaled * normed, axis=-1, keepdims=True)))
    d_three_b = d_three.astype(jnp.bfloat16)
    grad_w3 = matmul_tn(act_two, d_three_b)
    d_two = matmul_nt(d_three_b, rest_w[1]) * silu_grad(pre_two)
    d_two_b = d_two.astype(jnp.bfloat16)
    grad_w2 = matmul_tn(act_one, d_two_b)
    d_one = matmul_nt(d_two_b, rest_w[0]) * silu_grad(pre_one)
    d_one_b = d_one.astype(jnp.bfloat16)
    grad_w1 = matmul_tn(inputs, d_one_b)
    grad_in = matmul_nt(d_one_b, first_w)
    bias_grads = jnp.stack([lax.optimization_barrier(jnp.sum(d_one, axis=0)), lax.optimization_barrier(jnp.sum(d_two, axis=0)), lax.optimization_barrier(jnp.sum(d_three, axis=0)), grad_shift])
    return (grad_in, (grad_w1, jnp.stack([grad_w2, grad_w3]), bias_grads, grad_gain))

def edge_messages(weights, node_latents, latents, sources, targets, keep_rows, rows):

    def one_block(block):
        block_latents, block_sources, block_targets, block_keep = block
        inputs = jnp.concatenate([block_latents, node_latents[block_sources], node_latents[block_targets]], axis=1)
        message, _ = mlp_parts(inputs, *weights)
        return message * block_keep[:, None]
    blocks = (latents.reshape(-1, rows, D), sources.reshape(-1, rows), targets.reshape(-1, rows), keep_rows.reshape(-1, rows))
    return lax.map(one_block, blocks).reshape(-1, D)

def edge_gradients(weights, node_latents, latents, sources, targets, keep_rows, cotangent, upstream_nodes, grad_nodes, rows):

    def one_block(carried, block):
        running, grad_sums = carried
        block_latents, block_sources, block_targets, block_keep, block_cot = block
        inputs = jnp.concatenate([block_latents, node_latents[block_sources], node_latents[block_targets]], axis=1)
        incoming_cot = block_cot.astype(jnp.float32)
        upstream = block_keep[:, None] * (incoming_cot + upstream_nodes[block_targets])
        in_grad, weight_grads = mlp_backward(inputs, *weights, upstream)
        running = running.at[block_sources].add(in_grad[:, D:2 * D]).at[block_targets].add(in_grad[:, 2 * D:])
        grad_sums = jax.tree.map(jnp.add, grad_sums, weight_grads)
        return ((running, grad_sums), (incoming_cot + in_grad[:, :D]).astype(jnp.bfloat16))
    empty_grads = (jnp.zeros((3 * D, D), jnp.float32), jnp.zeros((2, D, D), jnp.float32), jnp.zeros((4, D), jnp.float32), jnp.zeros((D,), jnp.float32))
    blocks = (latents.reshape(-1, rows, D), sources.reshape(-1, rows), targets.reshape(-1, rows), keep_rows.reshape(-1, rows), cotangent.reshape(-1, rows, D))
    (grad_nodes, grad_sums), own_grads = lax.scan(one_block, (grad_nodes, empty_grads), blocks)
    return (grad_nodes, grad_sums, own_grads.reshape(-1, D))

def reference(node_latents, mesh_latents, world_latents, mesh_src, mesh_dst, world_src, world_dst, send_blocks, world_count, node_cot, mesh_cot, world_cot, first_weights, rest_weights, biases, gains):
    device_count = N_DOM * N_DP
    node_count = node_latents.shape[0]
    weights = [(first_weights[which], rest_weights[which], biases[which], gains[which]) for which in range(3)]
    mesh_device = jnp.arange(mesh_src.shape[0], dtype=jnp.int32) // MEDGE_DEV
    offset = mesh_src - HALO
    neighbor_step = offset // NODE_DEV
    mesh_source = ((mesh_device + neighbor_step * N_DP) * NODE_DEV + offset - neighbor_step * NODE_DEV).astype(jnp.int32)
    mesh_target = (mesh_device * NODE_DEV + mesh_dst).astype(jnp.int32)
    mesh_keep = jnp.ones(mesh_src.shape, jnp.float32)
    world_index = jnp.arange(world_src.shape[0], dtype=jnp.int32)
    world_device = world_index // WEDGE_DEV
    peer_domain = world_src // (SLOTS * BLK)
    slot_index = world_src // BLK % SLOTS
    row_within = world_src % BLK
    owner = peer_domain * N_DP + world_device % N_DP
    chosen = send_blocks[owner, world_device // N_DP, slot_index]
    world_source = (owner * NODE_DEV + chosen * BLK + row_within).astype(jnp.int32)
    world_target = (world_device * NODE_DEV + world_dst).astype(jnp.int32)
    world_keep = (world_index % WEDGE_DEV < world_count[world_device]).astype(jnp.float32)
    mesh_message = edge_messages(weights[0], node_latents, mesh_latents, mesh_source, mesh_target, mesh_keep, MEDGE_DEV)
    world_message = edge_messages(weights[1], node_latents, world_latents, world_source, world_target, world_keep, WEDGE_DEV)
    new_mesh = (mesh_latents.astype(jnp.float32) + mesh_message).astype(jnp.bfloat16)
    new_world = (world_latents.astype(jnp.float32) + world_message).astype(jnp.bfloat16)
    mesh_sum = jax.ops.segment_sum(mesh_message, mesh_target, num_segments=node_count)
    world_sum = jax.ops.segment_sum(world_message, world_target, num_segments=node_count)
    node_input = jnp.concatenate([node_latents, mesh_sum.astype(jnp.bfloat16), world_sum.astype(jnp.bfloat16)], axis=1)
    node_update, _ = mlp_parts(node_input, *weights[2])
    new_nodes = (node_latents.astype(jnp.float32) + node_update).astype(jnp.bfloat16)
    node_back, node_grads = mlp_backward(node_input, *weights[2], node_cot.astype(jnp.float32))
    grad_nodes = node_cot.astype(jnp.float32) + node_back[:, :D]
    mesh_back = node_back[:, D:2 * D]
    world_back = node_back[:, 2 * D:]
    grad_nodes, mesh_grads, grad_mesh = edge_gradients(weights[0], node_latents, mesh_latents, mesh_source, mesh_target, mesh_keep, mesh_cot, mesh_back, grad_nodes, MEDGE_DEV)
    grad_nodes, world_grads, grad_world = edge_gradients(weights[1], node_latents, world_latents, world_source, world_target, world_keep, world_cot, world_back, grad_nodes, WEDGE_DEV)
    summed_all = [jnp.stack([mesh_grads[which], world_grads[which], node_grads[which]]) / device_count for which in range(4)]
    return (new_nodes, new_mesh, new_world, grad_nodes.astype(jnp.bfloat16), grad_mesh, grad_world, summed_all[0], summed_all[1], summed_all[2], summed_all[3])
```

```python
import functools

import jax
import jax.numpy as jnp
from jax import lax
from jax.experimental import pallas as pl
from jax.experimental.pallas import tpu as pltpu
from jax.sharding import PartitionSpec as P

HALO = 256
BLK = 16
LANES = 128
PACK = 656

norm_eps = 1e-05
f32 = jnp.float32
bf16 = jnp.bfloat16


def dot(left, right):
    return jnp.dot(left, right, preferred_element_type=f32)


def dot_nt(left, right):
    return lax.dot_general(left, right, (((1,), (1,)), ((), ())), preferred_element_type=f32)


def dot_tn(left, right):
    return lax.dot_general(left, right, (((0,), (0,)), ((), ())), preferred_element_type=f32)


def sigmoid(values):
    return 0.5 * jnp.tanh(0.5 * values) + 0.5


def split(values):
    high = values.astype(bf16)
    low = (values - high.astype(f32)).astype(bf16)
    return jnp.concatenate([high, low], axis=1)


def joined(values):
    half = values.shape[1] // 2
    return values[:, :half] + values[:, half:]


def hot_rows(index, width):
    parts = []
    iota = lax.broadcasted_iota(jnp.int32, (LANES, width), 1)
    for row in range(index.shape[0]):
        column = jnp.broadcast_to(index[row : row + 1], (LANES, LANES)).T
        wide = jnp.concatenate([column] * (width // LANES), axis=1)
        parts.append(jnp.where(wide == iota, 1.0, 0.0).astype(bf16))
    return jnp.concatenate(parts, axis=0)


def hot_cols(index, first, width):
    iota = lax.broadcasted_iota(jnp.int32, (width, LANES), 0) + first
    parts = [
        jnp.where(jnp.broadcast_to(index[row : row + 1], (width, LANES)) == iota, 1.0, 0.0).astype(bf16)
        for row in range(index.shape[0])
    ]
    return jnp.concatenate(parts, axis=1)


def upper_layers(pre_one, rest_w, bias, gain):
    act_one = (pre_one * sigmoid(pre_one)).astype(bf16)
    pre_two = dot(act_one, rest_w[0]) + bias[1:2]
    act_two = (pre_two * sigmoid(pre_two)).astype(bf16)
    pre_three = dot(act_two, rest_w[1]) + bias[2:3]
    centred = pre_three - jnp.mean(pre_three, axis=-1, keepdims=True)
    inv_std = lax.rsqrt(jnp.mean(centred * centred, axis=-1, keepdims=True) + norm_eps)
    normed = centred * inv_std
    return normed * gain + bias[3:4], pre_two, normed, inv_std


def silu_parts(values):
    sigma = sigmoid(values)
    return (values * sigma).astype(bf16), sigma * (1.0 + values * (1.0 - sigma))


def backward_layers(cotangent, pre_one, pre_two, normed, inv_std, rest_w, gain):
    grad_gain = jnp.sum(cotangent * normed, axis=0, keepdims=True)
    grad_shift = jnp.sum(cotangent, axis=0, keepdims=True)
    scaled = cotangent * gain
    d_three = inv_std * (
        scaled
        - jnp.mean(scaled, axis=-1, keepdims=True)
        - normed * jnp.mean(scaled * normed, axis=-1, keepdims=True)
    )
    d_three_b = d_three.astype(bf16)
    act_two, slope_two = silu_parts(pre_two)
    grad_w3 = dot_tn(act_two, d_three_b)
    d_two = dot_nt(d_three_b, rest_w[1]) * slope_two
    d_two_b = d_two.astype(bf16)
    act_one, slope_one = silu_parts(pre_one)
    grad_w2 = dot_tn(act_one, d_two_b)
    d_one = dot_nt(d_two_b, rest_w[0]) * slope_one
    small = jnp.concatenate(
        [jnp.sum(d, axis=0, keepdims=True) for d in (d_one, d_two, d_three)] + [grad_shift, grad_gain],
        axis=0,
    )
    return d_one.astype(bf16), grad_w2, grad_w3, small


def send_kernel(blocks_ref, node_ref, out_ref):
    def one(step, _):
        source = pl.multiple_of(blocks_ref[step] * BLK, BLK)
        target = pl.multiple_of(step * BLK, BLK)
        out_ref[pl.ds(target, BLK), :] = node_ref[pl.ds(source, BLK), :]
        return 0

    lax.fori_loop(0, out_ref.shape[0] // BLK, one, 0, unroll=8)


def mesh_forward_kernel(
    lat_ref, before_ref, node_ref, after_ref, src_ref, dst_ref, first_ref, rest_ref, bias_ref, gain_ref,
    new_ref, one_ref, two_ref, norm_ref, inv_ref, sum_ref,
    table_src, table_dst, message_ref,
):
    tiles, groups = src_ref.shape[:2]
    tile = groups * LANES
    width = lat_ref.shape[1]
    nodes = node_ref.shape[0]
    halo = before_ref.shape[0]
    w_own = first_ref[0, :width]
    w_src = first_ref[0, width : 2 * width]
    w_dst = first_ref[0, 2 * width :]
    bias = bias_ref[0]
    gain = gain_ref[0:1]
    rest = (rest_ref[0, 0], rest_ref[0, 1])
    table_src[:halo] = split(dot(before_ref[...], w_src))
    table_src[halo : halo + nodes] = split(dot(node_ref[...], w_src))
    table_src[halo + nodes :] = split(dot(after_ref[...], w_src))
    table_dst[...] = split(dot(node_ref[...], w_dst))

    def one(step, _):
        rows = pl.ds(pl.multiple_of(step * tile, tile), tile)
        own = lat_ref[rows, :]
        gathered = dot(hot_rows(src_ref[step], nodes + 2 * halo), table_src[...])
        gathered = gathered + dot(hot_rows(dst_ref[step], nodes), table_dst[...])
        pre_one = dot(own, w_own) + joined(gathered) + bias[0:1]
        message, pre_two, normed, inv_std = upper_layers(pre_one, rest, bias, gain)
        new_ref[rows, :] = (own.astype(f32) + message).astype(bf16)
        one_ref[rows, :] = pre_one
        two_ref[rows, :] = pre_two
        norm_ref[rows, :] = normed
        inv_ref[rows, :] = jnp.broadcast_to(inv_std, normed.shape)
        message_ref[rows, :] = split(message)
        return 0

    lax.fori_loop(0, tiles, one, 0)
    block = 256

    def total(step, _):
        first = pl.multiple_of(step * block, block)
        hot = jnp.concatenate([hot_cols(dst_ref[t], first, block) for t in range(tiles)], axis=1)
        sum_ref[pl.ds(first, block), :] = joined(dot(hot, message_ref[...])).astype(bf16)
        return 0

    lax.fori_loop(0, nodes // block, total, 0)


def write_pack(ref, start, grad_first, grad_w2, grad_w3, small):
    wide, width = grad_first.shape
    ref[start : start + wide, :] = grad_first.astype(bf16)
    ref[start + wide : start + wide + width, :] = grad_w2.astype(bf16)
    ref[start + wide + width : start + wide + 2 * width, :] = grad_w3.astype(bf16)
    zeros = jnp.zeros((BLK - small.shape[0], width), f32)
    tail = start + wide + 2 * width
    ref[tail : tail + BLK, :] = jnp.concatenate([small, zeros], axis=0).astype(bf16)


def middle_kernel(
    count_ref, node_ref, lat_ref, incoming_ref, src_ref, dst_ref, sum_ref, node_cot_ref, world_cot_ref,
    first_ref, rest_ref, bias_ref, gain_ref,
    new_nodes_ref, new_world_ref, grad_world_ref, source_ref, local_ref, back_ref, pack_ref,
):
    nodes, width = node_ref.shape
    rows = lat_ref.shape[0]
    received = incoming_ref.shape[0]
    node = node_ref[...]
    keep = (lax.broadcasted_iota(jnp.int32, (rows, 1), 0) < count_ref[0]).astype(f32)

    src = src_ref[...]
    dst = dst_ref[...]
    lat = lat_ref[...]
    hot_dst = hot_rows(dst, nodes)
    x_src = dot(hot_rows(src, received), incoming_ref[...]).astype(bf16)
    x_dst = dot(hot_dst, node).astype(bf16)
    w_inputs = jnp.concatenate([lat, x_src, x_dst], axis=1)
    w_rest = (rest_ref[1, 0], rest_ref[1, 1])
    w_one = dot(w_inputs, first_ref[1]) + bias_ref[1][0:1]
    message, w_two, w_norm, w_inv = upper_layers(w_one, w_rest, bias_ref[1], gain_ref[1:2])
    message = message * keep
    new_world_ref[...] = (lat.astype(f32) + message).astype(bf16)
    world_sum = joined(dot(hot_cols(dst, 0, nodes), split(message))).astype(bf16)

    n_inputs = jnp.concatenate([node, sum_ref[...], world_sum], axis=1)
    n_rest = (rest_ref[2, 0], rest_ref[2, 1])
    n_one = dot(n_inputs, first_ref[2]) + bias_ref[2][0:1]
    update, n_two, n_norm, n_inv = upper_layers(n_one, n_rest, bias_ref[2], gain_ref[2:3])
    new_nodes_ref[...] = (node.astype(f32) + update).astype(bf16)
    node_cot = node_cot_ref[...].astype(f32)
    d_one, grad_w2, grad_w3, small = backward_layers(
        node_cot, n_one, n_two, n_norm, n_inv, n_rest, gain_ref[2:3]
    )
    write_pack(pack_ref, PACK, dot_tn(n_inputs, d_one), grad_w2, grad_w3, small)
    node_back = dot_nt(d_one, first_ref[2])
    local_ref[...] = node_cot + node_back[:, :width]
    back_ref[...] = split(node_back[:, width : 2 * width])
    world_back = split(node_back[:, 2 * width :])

    world_cot = world_cot_ref[...].astype(f32)
    upstream = keep * (world_cot + joined(dot(hot_dst, world_back)))
    d_one, grad_w2, grad_w3, small = backward_layers(
        upstream, w_one, w_two, w_norm, w_inv, w_rest, gain_ref[1:2]
    )
    write_pack(pack_ref, 0, dot_tn(w_inputs, d_one), grad_w2, grad_w3, small)
    in_grad = dot_nt(d_one, first_ref[1])
    grad_world_ref[...] = (world_cot + in_grad[:, :width]).astype(bf16)
    to_source = split(in_grad[:, width : 2 * width])
    to_target = split(in_grad[:, 2 * width :])
    local_ref[...] += joined(dot(hot_cols(dst, 0, nodes), to_target))
    block = 512

    def back(step, _):
        first = pl.multiple_of(step * block, block)
        source_ref[pl.ds(first, block), :] = joined(dot(hot_cols(src_ref[...], first, block), to_source)).astype(bf16)
        return 0

    lax.fori_loop(0, received // block, back, 0)


def mesh_backward_kernel(
    lat_ref, before_ref, node_ref, after_ref, src_ref, dst_ref, cot_ref, back_ref,
    one_ref, two_ref, norm_ref, inv_ref, local_ref, first_ref, rest_ref, gain_ref,
    grad_ref, left_ref, right_ref, out_ref, pack_ref,
    d_ref, w1_acc, w2_acc, w3_acc, small_acc, sum_src,
):
    tiles, groups = src_ref.shape[:2]
    tile = groups * LANES
    width = lat_ref.shape[1]
    nodes = node_ref.shape[0]
    halo = before_ref.shape[0]
    w_own = first_ref[0, :width]
    w_src = first_ref[0, width : 2 * width]
    w_dst = first_ref[0, 2 * width :]
    gain = gain_ref[0:1]
    rest = (rest_ref[0, 0], rest_ref[0, 1])
    for ref in (w1_acc, w2_acc, w3_acc, small_acc):
        ref[...] = jnp.zeros(ref.shape, f32)

    def one(step, _):
        rows = pl.ds(pl.multiple_of(step * tile, tile), tile)
        cot = cot_ref[rows, :].astype(f32)
        upstream = cot + joined(dot(hot_rows(dst_ref[step], nodes), back_ref[...]))
        d_one, grad_w2, grad_w3, small = backward_layers(
            upstream, one_ref[rows, :], two_ref[rows, :], norm_ref[rows, :], inv_ref[rows, :], rest, gain
        )
        d_ref[rows, :] = d_one
        w1_acc[...] += dot_tn(lat_ref[rows, :], d_one)
        w2_acc[...] += grad_w2
        w3_acc[...] += grad_w3
        small_acc[0 : small.shape[0], :] += small
        grad_ref[rows, :] = (cot + dot_nt(d_one, w_own)).astype(bf16)
        return 0

    lax.fori_loop(0, tiles, one, 0)
    block = 256

    def scattered(index_ref, first):
        hot = jnp.concatenate([hot_cols(index_ref[t], first, block) for t in range(tiles)], axis=1)
        return split(dot(hot, d_ref[...]))

    def source(step, total):
        first = pl.multiple_of(step * block, block)
        sum_src[pl.ds(first, block), :] = scattered(src_ref, first)
        return total

    lax.fori_loop(0, (nodes + 2 * halo) // block, source, 0)

    def target(step, total):
        first = pl.multiple_of(step * block, block)
        here = pl.ds(first, block)
        sums = scattered(dst_ref, first)
        inner = sum_src[pl.ds(pl.multiple_of(first + halo, block), block), :]
        grad = dot_nt(sums[:, :width], w_dst) + dot_nt(sums[:, width:], w_dst)
        grad = grad + dot_nt(inner[:, :width], w_src) + dot_nt(inner[:, width:], w_src)
        out_ref[here, :] = local_ref[here, :] + grad
        return total + dot_tn(node_ref[here, :], sums)

    grad_dst = joined(lax.fori_loop(0, nodes // block, target, jnp.zeros((width, 2 * width), f32)))
    first_rows = sum_src[:halo]
    last_rows = sum_src[halo + nodes :]
    left_ref[...] = (dot_nt(first_rows[:, :width], w_src) + dot_nt(first_rows[:, width:], w_src)).astype(bf16)
    right_ref[...] = (dot_nt(last_rows[:, :width], w_src) + dot_nt(last_rows[:, width:], w_src)).astype(bf16)
    grad_src = dot_tn(before_ref[...], first_rows) + dot_tn(node_ref[...], sum_src[halo : halo + nodes])
    grad_src = joined(grad_src + dot_tn(after_ref[...], last_rows))
    grad_first = jnp.concatenate([w1_acc[...], grad_src, grad_dst], axis=0)
    write_pack(pack_ref, 0, grad_first, w2_acc[...], w3_acc[...], small_acc[0:5, :])


def final_kernel(blocks_ref, local_ref, left_ref, right_ref, returned_ref, out_ref, total_ref):
    nodes = local_ref.shape[0]
    halo = left_ref.shape[0]
    total_ref[...] = local_ref[...]
    total_ref[:halo] += left_ref[...].astype(f32)
    total_ref[nodes - halo :] += right_ref[...].astype(f32)

    def one(step, _):
        target = pl.ds(pl.multiple_of(blocks_ref[step] * BLK, BLK), BLK)
        source = pl.ds(pl.multiple_of(step * BLK, BLK), BLK)
        total_ref[target, :] += returned_ref[source, :].astype(f32)
        return 0

    lax.fori_loop(0, returned_ref.shape[0] // BLK, one, 0, unroll=8)
    out_ref[...] = total_ref[...].astype(bf16)


def call(kernel, outs, operands, scalars=0, scratch=(), name=None):
    specs = [pl.BlockSpec(memory_space=pltpu.SMEM)] * scalars
    specs += [pl.BlockSpec(memory_space=pltpu.VMEM)] * (len(operands) - scalars)
    return pl.pallas_call(
        kernel,
        out_shape=[jax.ShapeDtypeStruct(shape, kind) for shape, kind in outs],
        in_specs=specs,
        out_specs=[pl.BlockSpec(memory_space=pltpu.VMEM)] * len(outs),
        scratch_shapes=list(scratch),
        name=name,
    )(*operands)


def per_device(
    node_latents,
    mesh_latents,
    world_latents,
    mesh_src,
    mesh_dst,
    world_src,
    world_dst,
    send_blocks,
    world_count,
    node_cot,
    mesh_cot,
    world_cot,
    first_weights,
    rest_weights,
    biases,
    gains,
):
    nodes, width = node_latents.shape
    edges = mesh_latents.shape[0]
    world_rows = world_latents.shape[0]
    domains = lax.axis_size("dom")
    devices = domains * lax.axis_size("dp")
    both = ("dom", "dp")
    up = [(i, i + 1) for i in range(domains - 1)]
    down = [(j, i) for i, j in up]
    blocks = send_blocks.reshape(-1)
    received = blocks.shape[0] * BLK

    (outgoing,) = call(send_kernel, [((received, width), bf16)], (blocks, node_latents), scalars=1, name="send")
    incoming = lax.all_to_all(outgoing, "dom", split_axis=0, concat_axis=0, tiled=True)
    before = lax.ppermute(node_latents[nodes - HALO :], "dom", up)
    after = lax.ppermute(node_latents[:HALO], "dom", down)

    tile = 4 * LANES
    src = mesh_src.reshape(edges // tile, tile // LANES, LANES)
    dst = mesh_dst.reshape(edges // tile, tile // LANES, LANES)
    full = ((edges, width), f32)
    new_mesh, pre_one, pre_two, normed, inv_std, mesh_sum = call(
        mesh_forward_kernel,
        [((edges, width), bf16), full, full, full, full, ((nodes, width), bf16)],
        (mesh_latents, before, node_latents, after, src, dst, first_weights, rest_weights, biases, gains),
        scratch=[
            pltpu.VMEM((nodes + 2 * HALO, 2 * width), bf16),
            pltpu.VMEM((nodes, 2 * width), bf16),
            pltpu.VMEM((edges, 2 * width), bf16),
        ],
        name="mesh_forward",
    )
    new_nodes, new_world, grad_world, to_source, local, mesh_back, early = call(
        middle_kernel,
        [
            ((nodes, width), bf16),
            ((world_rows, width), bf16),
            ((world_rows, width), bf16),
            ((received, width), bf16),
            ((nodes, width), f32),
            ((nodes, 2 * width), bf16),
            ((2 * PACK, width), bf16),
        ],
        (
            world_count,
            node_latents,
            world_latents,
            incoming,
            world_src.reshape(-1, LANES),
            world_dst.reshape(-1, LANES),
            mesh_sum,
            node_cot,
            world_cot,
            first_weights,
            rest_weights,
            biases,
            gains,
        ),
        scalars=1,
        name="middle",
    )
    returned = lax.all_to_all(to_source, "dom", split_axis=0, concat_axis=0, tiled=True)
    grad_mesh, to_left, to_right, local, late = call(
        mesh_backward_kernel,
        [
            ((edges, width), bf16),
            ((HALO, width), bf16),
            ((HALO, width), bf16),
            ((nodes, width), f32),
            ((PACK, width), bf16),
        ],
        (
            mesh_latents,
            before,
            node_latents,
            after,
            src,
            dst,
            mesh_cot,
            mesh_back,
            pre_one,
            pre_two,
            normed,
            inv_std,
            local,
            first_weights,
            rest_weights,
            gains,
        ),
        scratch=[
            pltpu.VMEM((edges, width), bf16),
            pltpu.VMEM((width, width), f32),
            pltpu.VMEM((width, width), f32),
            pltpu.VMEM((width, width), f32),
            pltpu.VMEM((8, width), f32),
            pltpu.VMEM((nodes + 2 * HALO, 2 * width), bf16),
        ],
        name="mesh_backward",
    )
    from_right = lax.ppermute(to_left, "dom", down)
    from_left = lax.ppermute(to_right, "dom", up)

    share = -(-3 * PACK // devices)
    share = -(-share // 16) * 16
    padding = jnp.zeros((share * devices - 3 * PACK, width), bf16)
    packed = jnp.concatenate([late, early, padding], axis=0)
    parts = lax.all_to_all(packed, both, split_axis=0, concat_axis=0, tiled=True)
    mine = jnp.sum(parts.reshape(devices, share, width).astype(f32), axis=0).astype(bf16)
    spread = jnp.broadcast_to(mine[None], (devices, share, width)).reshape(devices * share, width)
    spread = lax.all_to_all(spread, both, split_axis=0, concat_axis=0, tiled=True)
    sums = spread[: 3 * PACK].reshape(3, PACK, width).astype(f32) / devices
    (grad_nodes,) = call(
        final_kernel,
        [((nodes, width), bf16)],
        (blocks, local, from_left, from_right, returned),
        scalars=1,
        scratch=[pltpu.VMEM((nodes, width), f32)],
        name="final",
    )
    wide = 3 * width
    return (
        new_nodes,
        new_mesh,
        new_world,
        grad_nodes,
        grad_mesh,
        grad_world,
        sums[:, :wide],
        sums[:, wide : wide + 2 * width].reshape(3, 2, width, width),
        sums[:, wide + 2 * width : wide + 2 * width + 4],
        sums[:, wide + 2 * width + 4],
    )


def solution(mesh):
    rows = P(("dom", "dp"), None)
    flat = P(("dom", "dp"))
    return jax.shard_map(
        per_device,
        mesh=mesh,
        in_specs=(
            rows,
            rows,
            rows,
            flat,
            flat,
            flat,
            flat,
            P(("dom", "dp"), None, None),
            flat,
            rows,
            rows,
            rows,
            P(),
            P(),
            P(),
            P(),
        ),
        out_specs=(rows, rows, rows, rows, rows, rows, P(), P(), P(), P()),
        check_vma=False,
    )
```

```python
import functools

import jax
import jax.numpy as jnp
from jax import lax
from jax.experimental import pallas as pl
from jax.experimental.pallas import tpu as pltpu
from jax.sharding import PartitionSpec as P


HALO = 256
BLK = 16
LANES = 128
PACK = 656
COST = 250

norm_eps = 1e-05
f32 = jnp.float32
bf16 = jnp.bfloat16


def dot(left, right):
    return jnp.dot(left, right, preferred_element_type=f32)


def dot_nt(left, right):
    return lax.dot_general(left, right, (((1,), (1,)), ((), ())), preferred_element_type=f32)


def dot_tn(left, right):
    return lax.dot_general(left, right, (((0,), (0,)), ((), ())), preferred_element_type=f32)


def sigmoid(values):
    return 0.5 * jnp.tanh(0.5 * values) + 0.5


def split(values):
    high = values.astype(bf16)
    low = (values - high.astype(f32)).astype(bf16)
    return jnp.concatenate([high, low], axis=1)


def joined(values):
    half = values.shape[1] // 2
    return values[:, :half] + values[:, half:]


def hot_rows(index, width):
    parts = []
    iota = lax.broadcasted_iota(jnp.int32, (LANES, width), 1)
    for row in range(index.shape[0]):
        column = jnp.broadcast_to(index[row : row + 1], (LANES, LANES)).T
        wide = jnp.concatenate([column] * (width // LANES), axis=1)
        parts.append(jnp.where(wide == iota, 1.0, 0.0).astype(bf16))
    return jnp.concatenate(parts, axis=0)


def hot_cols(index, first, width):
    iota = lax.broadcasted_iota(jnp.int32, (width, LANES), 0) + first
    parts = [
        jnp.where(jnp.broadcast_to(index[row : row + 1], (width, LANES)) == iota, 1.0, 0.0).astype(bf16)
        for row in range(index.shape[0])
    ]
    return jnp.concatenate(parts, axis=1)


def upper_layers(pre_one, rest_w, bias, gain):
    act_one = (pre_one * sigmoid(pre_one)).astype(bf16)
    pre_two = dot(act_one, rest_w[0]) + bias[1:2]
    act_two = (pre_two * sigmoid(pre_two)).astype(bf16)
    pre_three = dot(act_two, rest_w[1]) + bias[2:3]
    centred = pre_three - jnp.mean(pre_three, axis=-1, keepdims=True)
    inv_std = lax.rsqrt(jnp.mean(centred * centred, axis=-1, keepdims=True) + norm_eps)
    normed = centred * inv_std
    return normed * gain + bias[3:4], pre_two, normed, inv_std


def silu_parts(values):
    sigma = sigmoid(values)
    return (values * sigma).astype(bf16), sigma * (1.0 + values * (1.0 - sigma))


def backward_layers(cotangent, pre_one, pre_two, normed, inv_std, rest_w, gain):
    grad_gain = jnp.sum(cotangent * normed, axis=0, keepdims=True)
    grad_shift = jnp.sum(cotangent, axis=0, keepdims=True)
    scaled = cotangent * gain
    d_three = inv_std * (
        scaled
        - jnp.mean(scaled, axis=-1, keepdims=True)
        - normed * jnp.mean(scaled * normed, axis=-1, keepdims=True)
    )
    d_three_b = d_three.astype(bf16)
    act_two, slope_two = silu_parts(pre_two)
    grad_w3 = dot_tn(act_two, d_three_b)
    d_two = dot_nt(d_three_b, rest_w[1]) * slope_two
    d_two_b = d_two.astype(bf16)
    act_one, slope_one = silu_parts(pre_one)
    grad_w2 = dot_tn(act_one, d_two_b)
    d_one = dot_nt(d_two_b, rest_w[0]) * slope_one
    small = jnp.concatenate(
        [jnp.sum(d, axis=0, keepdims=True) for d in (d_one, d_two, d_three)] + [grad_shift, grad_gain],
        axis=0,
    )
    return d_one.astype(bf16), grad_w2, grad_w3, small


def send_kernel(blocks_ref, node_ref, out_ref):
    _, domains, slots = blocks_ref.shape

    def one(domain, _):
        for slot in range(slots):
            source = pl.multiple_of(blocks_ref[0, domain, slot] * BLK, BLK)
            target = pl.multiple_of((domain * slots + slot) * BLK, BLK)
            out_ref[pl.ds(target, BLK), :] = node_ref[pl.ds(source, BLK), :]
        return 0

    lax.fori_loop(0, domains, one, 0)


def mesh_forward_kernel(
    lat_ref, before_ref, node_ref, after_ref, src_ref, dst_ref, first_ref, rest_ref, bias_ref, gain_ref,
    new_ref, sum_ref, saved_refs,
    table_src, table_dst, message_ref, saves, sems,
):
    tiles, groups = src_ref.shape[:2]
    tile = groups * LANES
    width = lat_ref.shape[1]
    nodes = node_ref.shape[0]
    halo = before_ref.shape[0]
    w_own = first_ref[0, :width]
    w_src = first_ref[0, width : 2 * width]
    w_dst = first_ref[0, 2 * width :]
    bias = bias_ref[0]
    gain = gain_ref[0:1]
    rest = (rest_ref[0, 0], rest_ref[0, 1])
    table_src[:halo] = split(dot(before_ref[...], w_src))
    table_src[halo : halo + nodes] = split(dot(node_ref[...], w_src))
    table_src[halo + nodes :] = split(dot(after_ref[...], w_src))
    table_dst[...] = split(dot(node_ref[...], w_dst))

    def one(step, _):
        rows = pl.ds(pl.multiple_of(step * tile, tile), tile)
        own = lat_ref[rows, :]
        gathered = dot(hot_rows(src_ref[step], nodes + 2 * halo), table_src[...])
        gathered = gathered + dot(hot_rows(dst_ref[step], nodes), table_dst[...])
        pre_one = dot(own, w_own) + joined(gathered) + bias[0:1]
        message, pre_two, normed, inv_std = upper_layers(pre_one, rest, bias, gain)
        new_ref[rows, :] = (own.astype(f32) + message).astype(bf16)
        for which, value in enumerate((pre_one, pre_two, normed, jnp.broadcast_to(inv_std, normed.shape))):
            saves[which, rows, :] = value
            pltpu.make_async_copy(saves.at[which, rows], saved_refs.at[which, rows], sems.at[step, which]).start()
        message_ref[rows, :] = split(message)
        return 0

    lax.fori_loop(0, tiles, one, 0)
    block = 256

    def total(step, _):
        first = pl.multiple_of(step * block, block)
        hot = jnp.concatenate([hot_cols(dst_ref[t], first, block) for t in range(tiles)], axis=1)
        sum_ref[pl.ds(first, block), :] = joined(dot(hot, message_ref[...])).astype(bf16)
        return 0

    lax.fori_loop(0, nodes // block, total, 0)

    def finish(step, _):
        rows = pl.ds(pl.multiple_of(step * tile, tile), tile)
        for which in range(saves.shape[0]):
            pltpu.make_async_copy(saves.at[which, rows], saved_refs.at[which, rows], sems.at[step, which]).wait()
        return 0

    lax.fori_loop(0, tiles, finish, 0)


def write_pack(ref, start, grad_first, grad_w2, grad_w3, small):
    wide, width = grad_first.shape
    ref[start : start + wide, :] = grad_first.astype(bf16)
    ref[start + wide : start + wide + width, :] = grad_w2.astype(bf16)
    ref[start + wide + width : start + wide + 2 * width, :] = grad_w3.astype(bf16)
    zeros = jnp.zeros((BLK - small.shape[0], width), f32)
    tail = start + wide + 2 * width
    ref[tail : tail + BLK, :] = jnp.concatenate([small, zeros], axis=0).astype(bf16)


def middle_kernel(
    count_ref, node_ref, lat_ref, incoming_ref, src_ref, dst_ref, sum_ref, node_cot_ref, world_cot_ref,
    first_ref, rest_ref, bias_ref, gain_ref,
    new_nodes_ref, new_world_ref, grad_world_ref, source_ref, local_ref, back_ref, pack_ref,
):
    nodes, width = node_ref.shape
    rows = lat_ref.shape[0]
    received = incoming_ref.shape[0]
    node = node_ref[...]
    keep = (lax.broadcasted_iota(jnp.int32, (rows, 1), 0) < count_ref[0]).astype(f32)

    src = src_ref[...]
    dst = dst_ref[...]
    lat = lat_ref[...]
    hot_dst = hot_rows(dst, nodes)
    x_src = dot(hot_rows(src, received), incoming_ref[...]).astype(bf16)
    x_dst = dot(hot_dst, node).astype(bf16)
    w_inputs = jnp.concatenate([lat, x_src, x_dst], axis=1)
    w_rest = (rest_ref[1, 0], rest_ref[1, 1])
    w_one = dot(w_inputs, first_ref[1]) + bias_ref[1][0:1]
    message, w_two, w_norm, w_inv = upper_layers(w_one, w_rest, bias_ref[1], gain_ref[1:2])
    message = message * keep
    new_world_ref[...] = (lat.astype(f32) + message).astype(bf16)
    world_sum = joined(dot(hot_cols(dst, 0, nodes), split(message))).astype(bf16)

    n_inputs = jnp.concatenate([node, sum_ref[...], world_sum], axis=1)
    n_rest = (rest_ref[2, 0], rest_ref[2, 1])
    n_one = dot(n_inputs, first_ref[2]) + bias_ref[2][0:1]
    update, n_two, n_norm, n_inv = upper_layers(n_one, n_rest, bias_ref[2], gain_ref[2:3])
    new_nodes_ref[...] = (node.astype(f32) + update).astype(bf16)
    node_cot = node_cot_ref[...].astype(f32)
    d_one, grad_w2, grad_w3, small = backward_layers(
        node_cot, n_one, n_two, n_norm, n_inv, n_rest, gain_ref[2:3]
    )
    write_pack(pack_ref, PACK, dot_tn(n_inputs, d_one), grad_w2, grad_w3, small)
    node_back = dot_nt(d_one, first_ref[2])
    local_ref[...] = node_cot + node_back[:, :width]
    back_ref[...] = split(node_back[:, width : 2 * width])
    world_back = split(node_back[:, 2 * width :])

    world_cot = world_cot_ref[...].astype(f32)
    upstream = keep * (world_cot + joined(dot(hot_dst, world_back)))
    d_one, grad_w2, grad_w3, small = backward_layers(
        upstream, w_one, w_two, w_norm, w_inv, w_rest, gain_ref[1:2]
    )
    write_pack(pack_ref, 0, dot_tn(w_inputs, d_one), grad_w2, grad_w3, small)
    in_grad = dot_nt(d_one, first_ref[1])
    grad_world_ref[...] = (world_cot + in_grad[:, :width]).astype(bf16)
    to_source = split(in_grad[:, width : 2 * width])
    to_target = split(in_grad[:, 2 * width :])
    local_ref[...] += joined(dot(hot_cols(dst, 0, nodes), to_target))
    block = 512

    def back(step, _):
        first = pl.multiple_of(step * block, block)
        source_ref[pl.ds(first, block), :] = joined(dot(hot_cols(src_ref[...], first, block), to_source)).astype(bf16)
        return 0

    lax.fori_loop(0, received // block, back, 0)


def mesh_backward_kernel(
    lat_ref, dst_ref, cot_ref, back_ref, saved_refs, first_ref, rest_ref, gain_ref,
    grad_ref, d_ref, pack_ref,
    w1_acc, w2_acc, w3_acc, small_acc, saves, sems,
):
    tiles, groups = dst_ref.shape[:2]
    tile = groups * LANES
    width = lat_ref.shape[1]
    nodes = back_ref.shape[0]
    w_own = first_ref[0, :width]
    gain = gain_ref[0:1]
    rest = (rest_ref[0, 0], rest_ref[0, 1])

    def fetch(step, _):
        rows = pl.ds(pl.multiple_of(step * tile, tile), tile)
        for which in range(saves.shape[0]):
            pltpu.make_async_copy(saved_refs.at[which, rows], saves.at[which, rows], sems.at[step, which]).start()
        return 0

    lax.fori_loop(0, tiles, fetch, 0)
    for ref in (w1_acc, w2_acc, w3_acc, small_acc):
        ref[...] = jnp.zeros(ref.shape, f32)

    def one(step, _):
        rows = pl.ds(pl.multiple_of(step * tile, tile), tile)
        cot = cot_ref[rows, :].astype(f32)
        upstream = cot + joined(dot(hot_rows(dst_ref[step], nodes), back_ref[...]))
        for which in range(saves.shape[0]):
            pltpu.make_async_copy(saved_refs.at[which, rows], saves.at[which, rows], sems.at[step, which]).wait()
        saved = [saves[which, rows, :] for which in range(saves.shape[0])]
        d_one, grad_w2, grad_w3, small = backward_layers(upstream, *saved, rest, gain)
        d_ref[rows, :] = d_one
        w1_acc[...] += dot_tn(lat_ref[rows, :], d_one)
        w2_acc[...] += grad_w2
        w3_acc[...] += grad_w3
        small_acc[0 : small.shape[0], :] += small
        grad_ref[rows, :] = (cot + dot_nt(d_one, w_own)).astype(bf16)
        return 0

    lax.fori_loop(0, tiles, one, 0)
    write_pack(pack_ref, 0, w1_acc[...], w2_acc[...], w3_acc[...], small_acc[0:5, :])


def mesh_sums_kernel(
    me_ref, before_ref, node_ref, after_ref, src_ref, dst_ref, d_ref, local_ref, first_ref, own_ref, early_ref,
    left_ref, right_ref, out_ref, keep_ref, give_ref,
    sum_src, pack_ref,
):
    tiles = src_ref.shape[0]
    nodes, width = node_ref.shape
    halo = before_ref.shape[0]
    w_src = first_ref[0, width : 2 * width]
    w_dst = first_ref[0, 2 * width :]
    block = 256

    def scattered(index_ref, first):
        hot = jnp.concatenate([hot_cols(index_ref[t], first, block) for t in range(tiles)], axis=1)
        return split(dot(hot, d_ref[...]))

    def source(step, total):
        first = pl.multiple_of(step * block, block)
        sum_src[pl.ds(first, block), :] = scattered(src_ref, first)
        return total

    lax.fori_loop(0, (nodes + 2 * halo) // block, source, 0)

    def target(step, total):
        first = pl.multiple_of(step * block, block)
        here = pl.ds(first, block)
        sums = scattered(dst_ref, first)
        inner = sum_src[pl.ds(pl.multiple_of(first + halo, block), block), :]
        grad = dot_nt(sums[:, :width], w_dst) + dot_nt(sums[:, width:], w_dst)
        grad = grad + dot_nt(inner[:, :width], w_src) + dot_nt(inner[:, width:], w_src)
        out_ref[here, :] = local_ref[here, :] + grad
        return total + dot_tn(node_ref[here, :], sums)

    grad_dst = joined(lax.fori_loop(0, nodes // block, target, jnp.zeros((width, 2 * width), f32)))
    first_rows = sum_src[:halo]
    last_rows = sum_src[halo + nodes :]
    left_ref[...] = (dot_nt(first_rows[:, :width], w_src) + dot_nt(first_rows[:, width:], w_src)).astype(bf16)
    right_ref[...] = (dot_nt(last_rows[:, :width], w_src) + dot_nt(last_rows[:, width:], w_src)).astype(bf16)
    grad_src = dot_tn(before_ref[...], first_rows) + dot_tn(node_ref[...], sum_src[halo : halo + nodes])
    grad_src = joined(grad_src + dot_tn(after_ref[...], last_rows))
    pack_ref[:width, :] = own_ref[:width, :]
    pack_ref[width : 2 * width, :] = grad_src.astype(bf16)
    pack_ref[2 * width : 3 * width, :] = grad_dst.astype(bf16)
    pack_ref[3 * width : PACK, :] = own_ref[width:, :]
    pack_ref[PACK : 3 * PACK, :] = early_ref[...]
    pack_ref[3 * PACK :, :] = jnp.zeros((pack_ref.shape[0] - 3 * PACK, width), bf16)
    half = keep_ref.shape[0]
    keep_ref[...] = pack_ref[pl.ds(pl.multiple_of(me_ref[0] * half, half), half), :]
    give_ref[...] = pack_ref[pl.ds(pl.multiple_of((1 - me_ref[0]) * half, half), half), :]


def share_kernel(parts_ref, out_ref):
    total = jnp.sum(parts_ref[...].astype(f32), axis=0, keepdims=True).astype(bf16)
    out_ref[...] = jnp.broadcast_to(total, out_ref.shape)


def unpack_kernel(me_ref, mine_ref, theirs_ref, first_ref, rest_ref, bias_ref, gain_ref, ref, *, scale):
    half, width = mine_ref.shape
    ref[pl.ds(pl.multiple_of(me_ref[0] * half, half), half), :] = mine_ref[...]
    ref[pl.ds(pl.multiple_of((1 - me_ref[0]) * half, half), half), :] = theirs_ref[...]
    wide = 3 * width
    for which in range(3):
        start = which * PACK
        first_ref[which] = ref[start : start + wide, :].astype(f32) * scale
        rest_ref[which, 0] = ref[start + wide : start + wide + width, :].astype(f32) * scale
        rest_ref[which, 1] = ref[start + wide + width : start + wide + 2 * width, :].astype(f32) * scale
        small = ref[start + wide + 2 * width : start + PACK, :].astype(f32) * scale
        bias_ref[which] = small[:4]
        gain_ref[which : which + 1, :] = small[4:5]


def final_kernel(blocks_ref, local_ref, left_ref, right_ref, returned_ref, out_ref, total_ref):
    nodes = local_ref.shape[0]
    halo = left_ref.shape[0]
    total_ref[...] = local_ref[...]
    total_ref[:halo] += left_ref[...].astype(f32)
    total_ref[nodes - halo :] += right_ref[...].astype(f32)

    _, domains, slots = blocks_ref.shape

    def one(domain, _):
        for slot in range(slots):
            target = pl.ds(pl.multiple_of(blocks_ref[0, domain, slot] * BLK, BLK), BLK)
            source = pl.ds(pl.multiple_of((domain * slots + slot) * BLK, BLK), BLK)
            total_ref[target, :] += returned_ref[source, :].astype(f32)
        return 0

    lax.fori_loop(0, domains, one, 0)
    out_ref[...] = total_ref[...].astype(bf16)


def call(kernel, outs, operands, scalars=0, outside=(), scratch=(), cost=0):
    def place(where, scalar, hbm):
        return pl.BlockSpec(memory_space=pltpu.SMEM if where < scalar else pltpu.HBM if hbm else pltpu.VMEM)

    operands = [
        pltpu.with_memory_space_constraint(value, pltpu.HBM) if where in outside else value
        for where, value in enumerate(operands)
    ]
    return pl.pallas_call(
        kernel,
        out_shape=[pltpu.HBM(*out[:2]) if len(out) > 2 else jax.ShapeDtypeStruct(*out) for out in outs],
        in_specs=[place(where, scalars, where in outside) for where in range(len(operands))],
        out_specs=[place(0, 0, len(out) > 2) for out in outs],
        scratch_shapes=list(scratch),
        cost_estimate=pl.CostEstimate(flops=cost, transcendentals=0, bytes_accessed=0),
    )(*operands)


def exchange(value, axes, groups=None):
    return lax.all_to_all(value, axes, split_axis=0, concat_axis=0, axis_index_groups=groups, tiled=True)


def shift(value, pairs, axes="dom"):
    return lax.ppermute(value, axes, pairs)


def step(
    node_latents,
    mesh_latents,
    world_latents,
    mesh_src,
    mesh_dst,
    world_src,
    world_dst,
    send_blocks,
    world_count,
    node_cot,
    mesh_cot,
    world_cot,
    first_weights,
    rest_weights,
    biases,
    gains,
):
    nodes, width = node_latents.shape
    edges = mesh_latents.shape[0]
    world_rows = world_latents.shape[0]
    domains = lax.axis_size("dom")
    devices = domains * lax.axis_size("dp")
    both = ("dom", "dp")
    up = [(i, i + 1) for i in range(domains - 1)]
    down = [(j, i) for i, j in up]
    blocks = send_blocks
    received = blocks.shape[1] * blocks.shape[2] * BLK
    micro = 1000000 * COST

    share = -(-3 * PACK // (8 * devices)) * 8
    half = share * devices // 2
    me = (lax.axis_index(both) % 2).astype(jnp.int32).reshape(1)
    pairs = [(i, i ^ 1) for i in range(devices)]
    groups = [list(range(first, devices, 2)) for first in range(2)]

    (outgoing,) = call(send_kernel, [((received, width), bf16)], (blocks, node_latents), scalars=1, cost=2 * micro)
    incoming = exchange(outgoing, "dom")
    before = shift(node_latents[nodes - HALO :], up)
    after = shift(node_latents[:HALO], down)

    tile = 8 * LANES
    src = mesh_src.reshape(edges // tile, tile // LANES, LANES)
    dst = mesh_dst.reshape(edges // tile, tile // LANES, LANES)
    saves = (4, edges, width)
    new_mesh, mesh_sum, saved = call(
        mesh_forward_kernel,
        [((edges, width), bf16), ((nodes, width), bf16), (saves, f32, True)],
        (mesh_latents, before, node_latents, after, src, dst, first_weights, rest_weights, biases, gains),
        scratch=[
            pltpu.VMEM((nodes + 2 * HALO, 2 * width), bf16),
            pltpu.VMEM((nodes, 2 * width), bf16),
            pltpu.VMEM((edges, 2 * width), bf16),
            pltpu.VMEM(saves, f32),
            pltpu.SemaphoreType.DMA((edges // tile, saves[0])),
        ],
        cost=15 * micro,
    )
    new_nodes, new_world, grad_world, to_source, local, mesh_back, early = call(
        middle_kernel,
        [
            ((nodes, width), bf16),
            ((world_rows, width), bf16),
            ((world_rows, width), bf16),
            ((received, width), bf16),
            ((nodes, width), f32),
            ((nodes, 2 * width), bf16),
            ((2 * PACK, width), bf16),
        ],
        (
            world_count,
            node_latents,
            world_latents,
            incoming,
            world_src.reshape(-1, LANES),
            world_dst.reshape(-1, LANES),
            mesh_sum,
            node_cot,
            world_cot,
            first_weights,
            rest_weights,
            biases,
            gains,
        ),
        scalars=1,
        cost=10 * micro,
    )
    returned = exchange(to_source, "dom")
    grad_mesh, d_one, own_pack = call(
        mesh_backward_kernel,
        [((edges, width), bf16), ((edges, width), bf16), ((PACK - 2 * width, width), bf16)],
        (
            mesh_latents,
            dst,
            mesh_cot,
            mesh_back,
            saved,
            first_weights,
            rest_weights,
            gains,
        ),
        outside=(4,),
        scratch=[
            pltpu.VMEM((width, width), f32),
            pltpu.VMEM((width, width), f32),
            pltpu.VMEM((width, width), f32),
            pltpu.VMEM((8, width), f32),
            pltpu.VMEM(saves, f32),
            pltpu.SemaphoreType.DMA((edges // tile, saves[0])),
        ],
        cost=10 * micro,
    )
    to_left, to_right, local, keep, give = call(
        mesh_sums_kernel,
        [
            ((HALO, width), bf16),
            ((HALO, width), bf16),
            ((nodes, width), f32),
            ((half, width), bf16),
            ((half, width), bf16),
        ],
        (me, before, node_latents, after, src, dst, d_one, local, first_weights, own_pack, early),
        scalars=1,
        scratch=[pltpu.VMEM((nodes + 2 * HALO, 2 * width), bf16), pltpu.VMEM((2 * half, width), bf16)],
        cost=10 * micro,
    )
    from_right = shift(to_left, down)
    from_left = shift(to_right, up)
    got = shift(give, pairs, both)
    merged = (keep.astype(f32) + got.astype(f32)).astype(bf16)
    parts = exchange(merged, both, groups)
    shape = (devices // 2, share, width)
    (spread,) = call(share_kernel, [(shape, bf16)], (parts.reshape(shape),), cost=micro)
    mine = exchange(spread.reshape(merged.shape), both, groups)
    theirs = shift(mine, pairs, both)
    (grad_nodes,) = call(
        final_kernel,
        [((nodes, width), bf16)],
        (blocks, local, from_left, from_right, returned),
        scalars=1,
        scratch=[pltpu.VMEM((nodes, width), f32)],
        cost=2 * micro,
    )
    grads = call(
        functools.partial(unpack_kernel, scale=1.0 / devices),
        [((3, 3 * width, width), f32), ((3, 2, width, width), f32), ((3, 4, width), f32), ((3, width), f32)],
        (me, mine, theirs),
        scalars=1,
        scratch=[pltpu.VMEM((2 * half, width), bf16)],
        cost=micro,
    )
    return (
        new_nodes,
        new_mesh,
        new_world,
        grad_nodes,
        grad_mesh,
        grad_world,
        *grads,
    )


def solution(mesh):
    rows = P(("dom", "dp"), None)
    flat = P(("dom", "dp"))
    return jax.shard_map(
        step,
        mesh=mesh,
        in_specs=(
            rows,
            rows,
            rows,
            flat,
            flat,
            flat,
            flat,
            P(("dom", "dp"), None, None),
            flat,
            rows,
            rows,
            rows,
            P(),
            P(),
            P(),
            P(),
        ),
        out_specs=(rows, rows, rows, rows, rows, rows, P(), P(), P(), P()),
        check_vma=False,
    )
```
